512 devices in a mesh: row: 8 (over y_hi, core), col: 8 (over y_lo, x), depth: 8 (over z).
Axes of the slice: x: 4, y: 8 (y_hi: 4, y_lo: 2; y = y_hi * 2 + y_lo), z: 8, core: 2. Of those that a mesh axis runs over, the one named last changes fastest.
Arguments:
- inputs: bfloat16 [8, 512, 5120], P('depth', 'col', 'row'), may hold values from -6 to 6
- pre_act: bfloat16 [8, 512, 10240], P('depth', 'row', 'col'), may hold values from -8 to 8
- grad_out: bfloat16 [8, 512, 5120], P('depth', 'col', 'row'), may hold values from -6 to 6
- weight_up: bfloat16 [5120, 10240], P('row', 'col'), may hold values from -0.078125 to 0.078125
- weight_down: bfloat16 [10240, 5120], P('col', 'row'), may hold values from -0.0625 to 0.0625
Outputs:
- grad_inputs: bfloat16 [8, 512, 5120], P('depth', 'col', 'row')
- grad_up: float32 [5120, 10240], P('row', ('col', 'depth'))
- grad_down: float32 [10240, 5120], P(('col', 'depth'), 'row')
The draws below stay inside these ranges and needn't reach their ends.
All inputs are finite; a program needn't handle non-finite values.
Results may differ from the reference program's by a relative error of at most 0.02.
Values may be sent and summed in bfloat16 or wider, within the bound.
No kernel may reach another device: no remote copies, remote signals or barrier semaphores. Data moves between devices by JAX's collectives and lax.ppermute only.
A program may use at most 128 MiB of HBM per device.

```python
import jax
import jax.numpy as jnp
from jax import lax

D = 5120
FF = 10240
TOK_DEPTH = 512
N_ROW = 8
N_COL = 8
N_DEPTH = 8


def levels(key, extent, pieces, least, largest):
    loudness = 1.0
    for dim, parts in pieces:
        draws = jax.random.uniform(jax.random.fold_in(jax.random.fold_in(key, 6), dim), (parts,), jnp.float32, least / len(pieces), largest / len(pieces))
        loudness = loudness * jnp.repeat(jnp.exp(draws), extent[dim] // parts).reshape((-1,) + (1,) * (len(extent) - 1 - dim))
    return loudness


def noise(own_key, dims, width, bound, cuts=(), held_as=jnp.bfloat16):
    gain = levels(own_key, dims, cuts, -0.22, 0.18) if cuts else 1.0
    result = jax.random.normal(own_key, dims, jnp.float32) * width * gain
    return jnp.minimum(jnp.maximum(result, -bound), bound).astype(held_as)


def setup_inputs(seed: int = 0) -> dict:
    splits = jax.random.split(jax.random.key(seed), 6)
    inputs = noise(splits[0], (N_DEPTH, TOK_DEPTH, D), 1.0, 6.0, ((0, 8), (1, 8), (2, 8)))
    pre_act = noise(splits[1], (N_DEPTH, TOK_DEPTH, FF), 1.5, 8.0, ((0, 8), (1, 8), (2, 8)))
    grad_out = noise(splits[2], (N_DEPTH, TOK_DEPTH, D), 1.0, 6.0, ((0, 8), (1, 8), (2, 8)))
    weight_up = noise(splits[3], (D, FF), D ** -0.5, 0.078125, ((0, 8), (1, 8)))
    weight_down = noise(splits[4], (FF, D), FF ** -0.5, 0.0625, ((0, 8), (1, 8)))
    return dict(inputs=inputs, pre_act=pre_act, grad_out=grad_out, weight_up=weight_up, weight_down=weight_down)


root_coeff = 0.7978845608028654
cubic_coeff = 0.044715


def gelu_parts(values):
    inner = root_coeff * (values + cubic_coeff * values * values * values)
    tangent = jnp.tanh(inner)
    active = 0.5 * values * (1.0 + tangent)
    slope = 0.5 * (1.0 + tangent) + 0.5 * values * (1.0 - tangent * tangent) * root_coeff * (1.0 + 3.0 * cubic_coeff * values * values)
    return active, slope


def rounded(values):
    return lax.optimization_barrier(values.astype(jnp.bfloat16)).astype(jnp.float32)


def reference(inputs, pre_act, grad_out, weight_up, weight_down):
    layers = inputs.shape[0]
    rows_in = inputs.reshape(-1, D)
    rows_grad = grad_out.reshape(-1, D)
    pre_values = pre_act.reshape(-1, FF).astype(jnp.float32)
    width_block = D // N_ROW
    hidden_grad = jnp.zeros((rows_in.shape[0], FF), jnp.float32)
    for index in range(N_ROW):
        lower = index * width_block
        upper = lower + width_block
        part = jnp.dot(rows_grad[:, lower:upper], weight_down[:, lower:upper].T, preferred_element_type=jnp.float32)
        hidden_grad = hidden_grad + rounded(part)
    active, slope = gelu_parts(pre_values)
    active_b = active.astype(jnp.bfloat16)
    hidden_delta = (hidden_grad * slope).astype(jnp.bfloat16)
    hidden_block = FF // N_COL
    input_grad = jnp.zeros((rows_in.shape[0], D), jnp.float32)
    for index in range(N_COL):
        lower = index * hidden_block
        upper = lower + hidden_block
        part = jnp.dot(hidden_delta[:, lower:upper], weight_up[:, lower:upper].T, preferred_element_type=jnp.float32)
        input_grad = input_grad + rounded(part)
    grad_inputs = input_grad.astype(jnp.bfloat16).reshape(layers, TOK_DEPTH, D)
    grad_up = jnp.zeros((D, FF), jnp.float32)
    grad_down = jnp.zeros((FF, D), jnp.float32)
    for layer in range(layers):
        lower = layer * TOK_DEPTH
        upper = lower + TOK_DEPTH
        grad_up = grad_up + rounded(jnp.dot(rows_in[lower:upper].T, hidden_delta[lower:upper], preferred_element_type=jnp.float32))
        grad_down = grad_down + rounded(jnp.dot(active_b[lower:upper].T, rows_grad[lower:upper], preferred_element_type=jnp.float32))
    return grad_inputs, grad_up, grad_down
```

```python
import jax
import jax.numpy as jnp
from jax import lax
from jax.sharding import Mesh, PartitionSpec as P

root_coeff = 0.7978845608028654
cubic_coeff = 0.044715

ROW = ("yhi", "core")
COL = ("ylo", "x")
SWAP = [(0, 1), (1, 0)]


def spread(value, axis):
    copies = jnp.broadcast_to(value, (lax.axis_size(axis), *value.shape))
    return lax.all_to_all(copies, axis, split_axis=0, concat_axis=0, tiled=True)


def exchanged(value, axis):
    return lax.all_to_all(value, axis, split_axis=0, concat_axis=0, tiled=True)


def summed(pieces):
    return jnp.sum(pieces.astype(jnp.float32), axis=0)


def gelu_parts(values):
    inner = root_coeff * (values + cubic_coeff * values * values * values)
    tangent = jnp.tanh(inner)
    active = 0.5 * values * (1.0 + tangent)
    slope = 0.5 * (1.0 + tangent) + 0.5 * values * (1.0 - tangent * tangent) * root_coeff * (
        1.0 + 3.0 * cubic_coeff * values * values
    )
    return (active, slope)


def contract_last(left, right):
    return lax.dot_general(
        left, right, (((1,), (1,)), ((), ())), preferred_element_type=jnp.float32
    )


def contract_first(left, right):
    return lax.dot_general(
        left, right, (((0,), (0,)), ((), ())), preferred_element_type=jnp.float32
    )


def halves(pieces, core):
    split = pieces.reshape(4, 2, *pieces.shape[1:])
    mine = lax.dynamic_index_in_dim(split, core, 1, keepdims=False)
    other = lax.dynamic_index_in_dim(split, 1 - core, 1, keepdims=False)
    return mine.reshape(-1, mine.shape[-1]), other.reshape(-1, other.shape[-1])


def swapped(value):
    return lax.ppermute(value, "core", SWAP)


def local(inputs, pre_act, grad_out, weight_up, weight_down):
    core = lax.axis_index("core")
    layer_grads = spread(grad_out[0], COL)
    active, slope = gelu_parts(pre_act[0].astype(jnp.float32))
    active_own = active.astype(jnp.bfloat16)
    grads_mine, grads_other = halves(layer_grads, core)
    away = contract_last(grads_other, weight_down).astype(jnp.bfloat16)
    back = swapped(away)
    kept = contract_last(grads_mine, weight_down)
    pair = (kept + back.astype(jnp.float32)).astype(jnp.bfloat16)
    hidden_grad = summed(exchanged(pair.reshape(4, -1, pair.shape[1]), "yhi"))
    delta_own = (hidden_grad * slope).astype(jnp.bfloat16)

    active_mine = spread(active_own, "yhi").reshape(-1, active_own.shape[1])
    active_other = swapped(active_mine)
    lower = contract_first(active_mine, grads_mine) + contract_first(active_other, grads_other)
    lower = lower.astype(jnp.bfloat16).reshape(8, -1, lower.shape[1])
    grad_down = summed(exchanged(lower, "depth"))

    layer_inputs = spread(inputs[0], COL)
    inputs_mine, inputs_other = halves(layer_inputs, core)
    delta_mine = spread(delta_own, "yhi").reshape(-1, delta_own.shape[1])
    delta_other = swapped(delta_mine)
    upper = contract_first(delta_mine, inputs_mine) + contract_first(delta_other, inputs_other)
    upper = upper.astype(jnp.bfloat16).reshape(8, -1, upper.shape[1])
    grad_up = summed(exchanged(upper, "depth")).T

    part_mine = contract_last(delta_mine, weight_up).astype(jnp.bfloat16)
    part_other = contract_last(delta_other, weight_up).astype(jnp.bfloat16)
    first = jnp.where(core == 0, part_mine, part_other).reshape(4, 64, -1)
    second = jnp.where(core == 0, part_other, part_mine).reshape(4, 64, -1)
    parts = jnp.stack([first, second], axis=1).reshape(8, 64, -1)
    grad_inputs = summed(exchanged(parts, COL)).astype(jnp.bfloat16)[None]
    return (grad_inputs, grad_up, grad_down)


def solution(mesh):
    fine = Mesh(mesh.devices.reshape(4, 2, 2, 4, 8), ("yhi", "core", "ylo", "x", "depth"))
    placed = (
        P("depth", COL, ROW),
        P("depth", ROW, COL),
        P("depth", COL, ROW),
        P(ROW, COL),
        P(COL, ROW),
    )
    return jax.shard_map(
        local,
        mesh=fine,
        in_specs=placed,
        out_specs=(
            P("depth", COL, ROW),
            P(ROW, (*COL, "depth")),
            P((*COL, "depth"), ROW),
        ),
        check_vma=False,
    )
```

```python
import jax
import jax.numpy as jnp
from jax import lax
from jax.experimental import pallas as pl
from jax.experimental.pallas import tpu as pltpu
from jax.sharding import Mesh, PartitionSpec as P

root_coeff = 0.7978845608028654
cubic_coeff = 0.044715

ROW = ("yhi", "core")
COL = ("ylo", "x")
SWAP = [(0, 1), (1, 0)]


def spread(value, axis):
    copies = jnp.broadcast_to(value, (lax.axis_size(axis), *value.shape))
    return lax.all_to_all(copies, axis, split_axis=0, concat_axis=0, tiled=True)


def exchanged(value, axis):
    return lax.all_to_all(value, axis, split_axis=0, concat_axis=0, tiled=True)


def summed(pieces):
    return jnp.sum(pieces.astype(jnp.float32), axis=0)


def gelu_parts(values):
    inner = root_coeff * (values + cubic_coeff * values * values * values)
    tangent = jnp.tanh(inner)
    active = 0.5 * values * (1.0 + tangent)
    slope = 0.5 * (1.0 + tangent) + 0.5 * values * (1.0 - tangent * tangent) * root_coeff * (
        1.0 + 3.0 * cubic_coeff * values * values
    )
    return (active, slope)


def contract_last(left, right):
    return lax.dot_general(
        left, right, (((1,), (1,)), ((), ())), preferred_element_type=jnp.float32
    )


def contract_first(left, right):
    return lax.dot_general(
        left, right, (((0,), (0,)), ((), ())), preferred_element_type=jnp.float32
    )


def shifted(value, axis, by):
    length = lax.axis_size(axis)
    return lax.ppermute(value, axis, [(k, (k + by) % length) for k in range(length)])


def swapped(value):
    return lax.ppermute(value, "core", SWAP)


def block_at(blocks, index):
    return lax.dynamic_index_in_dim(blocks, index, 0, keepdims=False)


def gathered(own):
    return jnp.concatenate([own] + [shifted(own, "yhi", 4 - u) for u in (1, 2, 3)], axis=0)


def depth_sum(blocks):
    here = lax.axis_index("depth")
    pick = lambda by: block_at(blocks, (here + by) % 8)
    half = blocks.shape[1] // 2
    far = pick(4)
    near_up = shifted(jnp.stack([pick(1), pick(3)]), "depth", 1)
    near_down = shifted(jnp.stack([pick(7), pick(5)]), "depth", 7)
    far_up = shifted(far[:half], "depth", 2)
    far_down = shifted(far[half:], "depth", 6)
    wide = lambda v: v.astype(jnp.float32)
    up = wide(pick(2)) + wide(near_up[1])
    up = jnp.concatenate([up[:half] + wide(far_up), up[half:]], axis=0).astype(jnp.bfloat16)
    down = wide(pick(6)) + wide(near_down[1])
    down = jnp.concatenate([down[:half], down[half:] + wide(far_down)], axis=0).astype(jnp.bfloat16)
    last_up = shifted(up, "depth", 2)
    last_down = shifted(down, "depth", 6)
    near = wide(pick(0)) + wide(near_up[0]) + wide(near_down[0])
    return near + wide(last_up) + wide(last_down)


def pick_kernel(order, blocks, *outs):
    for k in range(blocks.shape[0]):
        start = 0
        for out in outs:
            width = out.shape[-1]
            out[k] = blocks[order[k], :, start : start + width]
            start += width


def picked(blocks, order, ways=1):
    n, m, w = blocks.shape
    whole = pl.BlockSpec(memory_space=pltpu.VMEM)
    outs = pl.pallas_call(
        pick_kernel,
        out_shape=[jax.ShapeDtypeStruct((n, m, w // ways), blocks.dtype)] * ways,
        in_specs=[pl.BlockSpec(memory_space=pltpu.SMEM), whole],
        out_specs=[whole] * ways,
        name="pick",
    )(jnp.stack(order).astype(jnp.int32), blocks)
    return [out.reshape(n * m, w // ways) for out in outs]


def together(*values):
    return lax.optimization_barrier(values)


def local(inputs, pre_act, grad_out, weight_up, weight_down):
    core = lax.axis_index("core")
    high = lax.axis_index("yhi")
    active, slope = gelu_parts(pre_act[0].astype(jnp.float32))
    active_mine = gathered(active.astype(jnp.bfloat16))

    both = spread(jnp.concatenate([grad_out[0], inputs[0]], axis=1), COL)
    both, active_mine = together(both, active_mine)
    active_all = jnp.concatenate([active_mine, swapped(active_mine)], axis=0)
    order = [((high + u) % 4) * 2 + c for c in (core, 1 - core) for u in range(4)]
    grads, layer_inputs = picked(both, order, 2)

    away = contract_last(grads[256:], weight_down).astype(jnp.bfloat16)
    back = swapped(away)
    kept = contract_last(grads[:256], weight_down)
    pair = (kept + back.astype(jnp.float32)).astype(jnp.bfloat16).reshape(4, 64, -1)

    lower = contract_first(active_all, grads).astype(jnp.bfloat16)
    pair, lower = together(pair, lower)
    lower_pieces = exchanged(lower.reshape(8, -1, lower.shape[1]), "depth")

    came = [pair[0]] + [shifted(pair[u], "yhi", u) for u in (1, 2, 3)]
    hidden_grad = sum(piece.astype(jnp.float32) for piece in came)
    delta_mine = gathered((hidden_grad * slope).astype(jnp.bfloat16))
    delta_all = jnp.concatenate([delta_mine, swapped(delta_mine)], axis=0)
    delta_all, lower_pieces = together(delta_all, lower_pieces)
    grad_down = summed(lower_pieces)

    upper = contract_first(delta_all, layer_inputs).astype(jnp.bfloat16)
    grad_up = depth_sum(upper.reshape(8, -1, upper.shape[1])).T

    parts = contract_last(delta_all, weight_up).astype(jnp.bfloat16).reshape(8, 64, -1)
    spot = [(k // 2 - high) % 4 + 4 * ((k + core) % 2) for k in range(8)]
    parts = picked(parts, spot)[0].reshape(8, 64, -1)
    grad_inputs = summed(exchanged(parts, COL)).astype(jnp.bfloat16)[None]
    return (grad_inputs, grad_up, grad_down)


def solution(mesh):
    fine = Mesh(mesh.devices.reshape(4, 2, 2, 4, 8), ("yhi", "core", "ylo", "x", "depth"))
    placed = (
        P("depth", COL, ROW),
        P("depth", ROW, COL),
        P("depth", COL, ROW),
        P(ROW, COL),
        P(COL, ROW),
    )
    return jax.shard_map(
        local,
        mesh=fine,
        in_specs=placed,
        out_specs=(
            P("depth", COL, ROW),
            P(ROW, (*COL, "depth")),
            P((*COL, "depth"), ROW),
        ),
        check_vma=False,
    )
```

```python
import jax
import jax.numpy as jnp
from jax import lax
from jax.experimental import pallas as pl
from jax.experimental.pallas import tpu as pltpu
from jax.sharding import Mesh, PartitionSpec as P


root_coeff = 0.7978845608028654
cubic_coeff = 0.044715

ROW = ("yhi", "core")
COL = ("ylo", "x")
SWAP = [(0, 1), (1, 0)]


def spread(value, axis):
    copies = jnp.broadcast_to(value, (lax.axis_size(axis), *value.shape))
    return lax.all_to_all(copies, axis, split_axis=0, concat_axis=0, tiled=True)


def exchanged(value, axis):
    return lax.all_to_all(value, axis, split_axis=0, concat_axis=0, tiled=True)


def summed(pieces):
    return jnp.sum(pieces.astype(jnp.float32), axis=0)


def gelu_parts(values):
    inner = root_coeff * (values + cubic_coeff * values * values * values)
    tangent = jnp.tanh(inner)
    active = 0.5 * values * (1.0 + tangent)
    slope = 0.5 * (1.0 + tangent) + 0.5 * values * (1.0 - tangent * tangent) * root_coeff * (
        1.0 + 3.0 * cubic_coeff * values * values
    )
    return (active, slope)


def contract_last(left, right):
    return lax.dot_general(
        left, right, (((1,), (1,)), ((), ())), preferred_element_type=jnp.float32
    )


def contract_first(left, right):
    return lax.dot_general(
        left, right, (((0,), (0,)), ((), ())), preferred_element_type=jnp.float32
    )


def shifted(value, axis, by):
    length = lax.axis_size(axis)
    return lax.ppermute(value, axis, [(k, (k + by) % length) for k in range(length)])


def swapped(value):
    return lax.ppermute(value, "core", SWAP)


def block_at(blocks, index):
    return lax.dynamic_index_in_dim(blocks, index, 0, keepdims=False)


def gathered(own):
    return jnp.concatenate([own] + [shifted(own, "yhi", 4 - u) for u in (1, 2, 3)], axis=0)


def wide(value):
    return value.astype(jnp.float32)


def depth_sum(blocks):
    here = lax.axis_index("depth")
    pick = lambda by: block_at(blocks, (here + by) % 8)
    half = blocks.shape[1] // 2
    near_up = shifted(jnp.stack([pick(1), pick(3)]), "depth", 1)
    near_down = shifted(jnp.stack([pick(7), pick(5)]), "depth", 7)
    far = pick(4)
    far_up = shifted(far[:half], "depth", 2)
    far_down = shifted(far[half:], "depth", 6)
    up = wide(pick(2)) + wide(near_up[1])
    up = jnp.concatenate([up[:half] + wide(far_up), up[half:]], axis=0).astype(jnp.bfloat16)
    down = wide(pick(6)) + wide(near_down[1])
    down = jnp.concatenate([down[:half], down[half:] + wide(far_down)], axis=0).astype(jnp.bfloat16)
    last_up = shifted(up, "depth", 2)
    last_down = shifted(down, "depth", 6)
    near = wide(pick(0)) + wide(near_up[0]) + wide(near_down[0])
    return near + wide(last_up) + wide(last_down)


def pick_kernel(spot, blocks, *outs):
    width = outs[0].shape[-1]
    for u in range(4):
        row = 2 * ((spot[0] + u) % 4)
        for c, core in enumerate((spot[1], 1 - spot[1])):
            for k in range(2):
                outs[2 * c + k][u] = blocks[row + core, :, k * width : (k + 1) * width]


def picked(blocks, high, core):
    width = blocks.shape[2] // 2
    whole = pl.BlockSpec(memory_space=pltpu.VMEM)
    outs = pl.pallas_call(
        pick_kernel,
        out_shape=[jax.ShapeDtypeStruct((4, 64, width), blocks.dtype)] * 4,
        in_specs=[pl.BlockSpec(memory_space=pltpu.SMEM), whole],
        out_specs=[whole] * 4,
        name="pick",
    )(jnp.stack([high, core]).astype(jnp.int32), blocks)
    return [out.reshape(256, width) for out in outs]


def place_kernel(spot, mine, other, out):
    for u in range(4):
        row = 2 * ((spot[0] + u) % 4)
        out[row + spot[1]] = mine[u]
        out[row + 1 - spot[1]] = other[u]


def placed_by_row(mine, other, high, core):
    width = mine.shape[1]
    whole = pl.BlockSpec(memory_space=pltpu.VMEM)
    return pl.pallas_call(
        place_kernel,
        out_shape=jax.ShapeDtypeStruct((8, 64, width), mine.dtype),
        in_specs=[pl.BlockSpec(memory_space=pltpu.SMEM), whole, whole],
        out_specs=whole,
        name="place",
    )(jnp.stack([high, core]).astype(jnp.int32), mine.reshape(4, 64, width), other.reshape(4, 64, width))


def step(inputs, pre_act, grad_out, weight_up, weight_down):
    core = lax.axis_index("core")
    high = lax.axis_index("yhi")
    active, slope = gelu_parts(pre_act[0].astype(jnp.float32))
    active, slope = lax.optimization_barrier((active.astype(jnp.bfloat16), slope))
    active_mine = gathered(active)

    both = spread(jnp.concatenate([grad_out[0], inputs[0]], axis=1), COL)
    grads_mine, inputs_mine, grads_other, inputs_other = picked(both, high, core)

    away = contract_last(grads_other, weight_down).astype(jnp.bfloat16)
    back = swapped(away)
    kept = contract_last(grads_mine, weight_down)
    pair = (kept + wide(back)).astype(jnp.bfloat16).reshape(4, 64, -1)
    came = [shifted(pair[u], "yhi", u) for u in (1, 2, 3)]

    active_other = swapped(active_mine)
    lower_mine = lax.optimization_barrier(contract_first(active_mine, grads_mine))
    lower = (contract_first(active_other, grads_other) + lower_mine).astype(jnp.bfloat16)
    lower_pieces = exchanged(lower.reshape(8, -1, lower.shape[1]), "depth")

    hidden_grad = wide(pair[0]) + sum(wide(piece) for piece in came)
    delta_own = (hidden_grad * slope).astype(jnp.bfloat16)
    delta_mine = gathered(delta_own)
    delta_other = swapped(delta_mine)

    upper_mine = lax.optimization_barrier(contract_first(delta_mine, inputs_mine))
    upper = (contract_first(delta_other, inputs_other) + upper_mine).astype(jnp.bfloat16)
    grad_up = depth_sum(upper.reshape(8, -1, upper.shape[1]))

    parts_mine = contract_last(delta_mine, weight_up).astype(jnp.bfloat16)
    parts_other = contract_last(delta_other, weight_up).astype(jnp.bfloat16)
    parts = placed_by_row(parts_mine, parts_other, high, core)
    parts = exchanged(parts, COL)
    grad_inputs = summed(parts).astype(jnp.bfloat16)[None]
    grad_down = summed(lower_pieces)
    return (grad_inputs, grad_up.T, grad_down)


def solution(mesh):
    fine = Mesh(mesh.devices.reshape(4, 2, 2, 4, 8), ("yhi", "core", "ylo", "x", "depth"))
    placed = (
        P("depth", COL, ROW),
        P("depth", ROW, COL),
        P("depth", COL, ROW),
        P(ROW, COL),
        P(COL, ROW),
    )
    return jax.shard_map(
        step,
        mesh=fine,
        in_specs=placed,
        out_specs=(
            P("depth", COL, ROW),
            P(ROW, (*COL, "depth")),
            P((*COL, "depth"), ROW),
        ),
        check_vma=False,
    )
```

```python
import jax
import jax.numpy as jnp
from jax import lax
from jax.sharding import Mesh, PartitionSpec as P


root_coeff = 0.7978845608028654
cubic_coeff = 0.044715

ROW = ("yhi", "core")
COL = ("ylo", "x")
SWAP = [(0, 1), (1, 0)]


def spread(value, axis):
    copies = jnp.broadcast_to(value, (lax.axis_size(axis), *value.shape))
    return lax.all_to_all(copies, axis, split_axis=0, concat_axis=0, tiled=True)


def exchanged(value, axis):
    return lax.all_to_all(value, axis, split_axis=0, concat_axis=0, tiled=True)


def summed(pieces):
    return jnp.sum(pieces.astype(jnp.float32), axis=0)


def gelu_parts(values):
    inner = root_coeff * (values + cubic_coeff * values * values * values)
    tangent = jnp.tanh(inner)
    active = 0.5 * values * (1.0 + tangent)
    slope = 0.5 * (1.0 + tangent) + 0.5 * values * (1.0 - tangent * tangent) * root_coeff * (
        1.0 + 3.0 * cubic_coeff * values * values
    )
    return (active, slope)


def contract_last(left, right):
    return lax.dot_general(
        left, right, (((1,), (1,)), ((), ())), preferred_element_type=jnp.float32
    )


def contract_first(left, right):
    return lax.dot_general(
        left, right, (((0,), (0,)), ((), ())), preferred_element_type=jnp.float32
    )


def shifted(value, axis, by):
    length = lax.axis_size(axis)
    return lax.ppermute(value, axis, [(k, (k + by) % length) for k in range(length)])


def swapped(value):
    return lax.ppermute(value, "core", SWAP)


def block_at(blocks, index):
    return lax.dynamic_index_in_dim(blocks, index, 0, keepdims=False)


def gathered(own):
    return jnp.concatenate([own] + [shifted(own, "yhi", 4 - u) for u in (1, 2, 3)], axis=0)


def wide(value):
    return value.astype(jnp.float32)


def depth_parts(blocks):
    here = lax.axis_index("depth")
    pick = lambda by: block_at(blocks, (here + by) % 8)
    even = here % 2 == 0
    near_up = shifted(jnp.stack([pick(1), pick(3)]), "depth", 1)
    near_down = shifted(jnp.stack([pick(7), pick(5)]), "depth", 7)
    turns = [(k, (k + 2) % 8 if k % 2 == 0 else (k - 2) % 8) for k in range(8)]
    far = wide(lax.ppermute(pick(4), "depth", turns))
    up = wide(pick(2)) + wide(near_up[1]) + jnp.where(even, far, 0.0)
    down = wide(pick(6)) + wide(near_down[1]) + jnp.where(even, 0.0, far)
    last_up = shifted(up.astype(jnp.bfloat16), "depth", 2)
    last_down = shifted(down.astype(jnp.bfloat16), "depth", 6)
    near = wide(pick(0)) + wide(near_up[0]) + wide(near_down[0])
    return near, last_up, last_down


def total(parts):
    near, last_up, last_down = parts
    return near + wide(last_up) + wide(last_down)


def step(inputs, pre_act, grad_out, weight_up, weight_down):
    core = lax.axis_index("core")
    high = lax.axis_index("yhi")
    active, slope = gelu_parts(wide(pre_act[0]))
    active, slope = lax.optimization_barrier((active.astype(jnp.bfloat16), slope))
    active_mine = gathered(active)

    both = spread(jnp.concatenate([grad_out[0], inputs[0]], axis=1), COL)
    width = inputs.shape[2]
    both = both.reshape(4, 2, *both.shape[1:])
    of = lambda c: lax.dynamic_index_in_dim(both, c, 1, keepdims=False)
    mine, other = of(core), of(1 - core)
    flat = lambda blocks: blocks.reshape(-1, blocks.shape[-1])
    away = contract_last(flat(other[..., :width]), weight_down).astype(jnp.bfloat16)
    back = swapped(away)
    kept = contract_last(flat(mine[..., :width]), weight_down)
    pair = (kept + wide(back)).astype(jnp.bfloat16).reshape(4, 64, -1)
    came = exchanged(pair, "yhi")

    active_other = swapped(active_mine)
    turned = lambda blocks: jnp.concatenate([block_at(blocks, (high + u) % 4) for u in range(4)], axis=0)
    lower_mine = lax.optimization_barrier(contract_first(active_mine, turned(mine[..., :width])))
    lower = contract_first(active_other, turned(other[..., :width])) + lower_mine
    lower = lower.astype(jnp.bfloat16)
    lower_parts = depth_parts(lower.reshape(8, -1, lower.shape[1]))

    delta_own = (summed(came) * slope).astype(jnp.bfloat16)
    delta_mine = flat(spread(delta_own, "yhi"))
    delta_other = swapped(delta_mine)

    upper_mine = lax.optimization_barrier(contract_first(delta_mine, flat(mine[..., width:])))
    upper = contract_first(delta_other, flat(other[..., width:])) + upper_mine
    upper = upper.astype(jnp.bfloat16)
    near, last_up, last_down = depth_parts(upper.reshape(8, -1, upper.shape[1]))

    parts_mine = contract_last(delta_mine, weight_up).astype(jnp.bfloat16)
    parts_other = contract_last(delta_other, weight_up).astype(jnp.bfloat16)
    first = jnp.where(core == 0, parts_mine, parts_other).reshape(4, 64, -1)
    second = jnp.where(core == 0, parts_other, parts_mine).reshape(4, 64, -1)
    parts = jnp.stack([first, second], axis=1).reshape(8, 64, -1)
    parts = exchanged(parts, COL)
    grad_inputs = summed(parts).astype(jnp.bfloat16)[None]
    grad_down = total(lower_parts)
    grad_inputs, grad_down, last_up = lax.optimization_barrier((grad_inputs, grad_down, last_up))
    grad_up = total((near, last_up, last_down))
    return (grad_inputs, grad_up.T, grad_down)


def solution(mesh):
    fine = Mesh(mesh.devices.reshape(4, 2, 2, 4, 8), ("yhi", "core", "ylo", "x", "depth"))
    placed = (
        P("depth", COL, ROW),
        P("depth", ROW, COL),
        P("depth", COL, ROW),
        P(ROW, COL),
        P(COL, ROW),
    )
    return jax.shard_map(
        step,
        mesh=fine,
        in_specs=placed,
        out_specs=(
            P("depth", COL, ROW),
            P(ROW, (*COL, "depth")),
            P((*COL, "depth"), ROW),
        ),
        check_vma=False,
    )
```

```python
import jax
import jax.numpy as jnp
from jax import lax
from jax.sharding import Mesh, PartitionSpec as P


root_coeff = 0.7978845608028654
cubic_coeff = 0.044715

ROW = ("yhi", "core")
COL = ("ylo", "x")
SWAP = [(0, 1), (1, 0)]


def spread(value, axis):
    copies = jnp.broadcast_to(value, (lax.axis_size(axis), *value.shape))
    return lax.all_to_all(copies, axis, split_axis=0, concat_axis=0, tiled=True)


def exchanged(value, axis):
    return lax.all_to_all(value, axis, split_axis=0, concat_axis=0, tiled=True)


def summed(pieces):
    return jnp.sum(pieces.astype(jnp.float32), axis=0)


def gelu_parts(values):
    inner = root_coeff * (values + cubic_coeff * values * values * values)
    tangent = jnp.tanh(inner)
    active = 0.5 * values * (1.0 + tangent)
    slope = 0.5 * (1.0 + tangent) + 0.5 * values * (1.0 - tangent * tangent) * root_coeff * (
        1.0 + 3.0 * cubic_coeff * values * values
    )
    return (active, slope)


def contract_last(left, right):
    return lax.dot_general(
        left, right, (((1,), (1,)), ((), ())), preferred_element_type=jnp.float32
    )


def contract_first(left, right):
    return lax.dot_general(
        left, right, (((0,), (0,)), ((), ())), preferred_element_type=jnp.float32
    )


def shifted(value, axis, by):
    length = lax.axis_size(axis)
    return lax.ppermute(value, axis, [(k, (k + by) % length) for k in range(length)])


def swapped(value):
    return lax.ppermute(value, "core", SWAP)


def block_at(blocks, index):
    return lax.dynamic_index_in_dim(blocks, index, 0, keepdims=False)


def gathered(own):
    return jnp.concatenate([own] + [shifted(own, "yhi", 4 - u) for u in (1, 2, 3)], axis=0)


def wide(value):
    return value.astype(jnp.float32)


def depth_parts(blocks):
    here = lax.axis_index("depth")
    pick = lambda by: block_at(blocks, (here + by) % 8)
    even = here % 2 == 0
    near_up = shifted(jnp.stack([pick(1), pick(3)]), "depth", 1)
    near_down = shifted(jnp.stack([pick(7), pick(5)]), "depth", 7)
    turns = [(k, (k + 2) % 8 if k % 2 == 0 else (k - 2) % 8) for k in range(8)]
    far = lax.ppermute(pick(4), "depth", turns)
    up = wide(pick(2)) + wide(near_up[1]) + jnp.where(even, wide(far), 0.0)
    up, far = lax.optimization_barrier((up.astype(jnp.bfloat16), far))
    down = wide(pick(6)) + wide(near_down[1]) + jnp.where(even, 0.0, wide(far))
    last_up = shifted(up, "depth", 2)
    last_down = shifted(down.astype(jnp.bfloat16), "depth", 6)
    near = wide(pick(0)) + wide(near_up[0]) + wide(near_down[0])
    return near, last_up, last_down


def total(parts):
    near, last_up, last_down = parts
    return near + wide(last_up) + wide(last_down)


def step(inputs, pre_act, grad_out, weight_up, weight_down):
    core = lax.axis_index("core")
    high = lax.axis_index("yhi")
    active, slope = gelu_parts(wide(pre_act[0]))
    active, slope = lax.optimization_barrier((active.astype(jnp.bfloat16), slope))
    active_mine = gathered(active)

    both = spread(jnp.concatenate([grad_out[0], inputs[0]], axis=1), COL)
    width = inputs.shape[2]
    both = both.reshape(4, 2, *both.shape[1:])
    of = lambda c: lax.dynamic_index_in_dim(both, c, 1, keepdims=False)
    mine, other = of(core), of(1 - core)
    flat = lambda blocks: blocks.reshape(-1, blocks.shape[-1])
    away = contract_last(flat(other[..., :width]), weight_down).astype(jnp.bfloat16)
    back = swapped(away)
    kept = contract_last(flat(mine[..., :width]), weight_down)
    pair = (kept + wide(back)).astype(jnp.bfloat16).reshape(4, 64, -1)
    came = exchanged(pair, "yhi")

    active_other = swapped(active_mine)
    turned = lambda blocks: jnp.concatenate([block_at(blocks, (high + u) % 4) for u in range(4)], axis=0)
    lower_mine = lax.optimization_barrier(contract_first(active_mine, turned(mine[..., :width])))
    lower = contract_first(active_other, turned(other[..., :width])) + lower_mine
    lower = lower.astype(jnp.bfloat16)
    lower_parts = depth_parts(lower.reshape(8, -1, lower.shape[1]))

    delta_own = (sum(wide(came[k]) for k in range(4)) * slope).astype(jnp.bfloat16)
    delta_mine = flat(spread(delta_own, "yhi"))
    delta_other = swapped(delta_mine)

    upper_mine = lax.optimization_barrier(contract_first(delta_mine, flat(mine[..., width:])))
    upper = contract_first(delta_other, flat(other[..., width:])) + upper_mine
    upper = upper.astype(jnp.bfloat16)
    near, last_up, last_down = depth_parts(upper.reshape(8, -1, upper.shape[1]))
    near = lax.optimization_barrier(near)

    parts_mine = contract_last(delta_mine, weight_up).astype(jnp.bfloat16)
    parts_other = contract_last(delta_other, weight_up).astype(jnp.bfloat16)
    first = jnp.where(core == 0, parts_mine, parts_other).reshape(4, 64, -1)
    second = jnp.where(core == 0, parts_other, parts_mine).reshape(4, 64, -1)
    parts = jnp.stack([first, second], axis=1).reshape(8, 64, -1)
    parts = exchanged(parts, COL)
    grad_inputs = summed(parts).astype(jnp.bfloat16)[None]
    grad_down = total(lower_parts)
    grad_inputs, grad_down, last_up = lax.optimization_barrier((grad_inputs, grad_down, last_up))
    grad_up = total((near, last_up, last_down))
    return (grad_inputs, grad_up.T, grad_down)


def solution(mesh):
    fine = Mesh(mesh.devices.reshape(4, 2, 2, 4, 8), ("yhi", "core", "ylo", "x", "depth"))
    placed = (
        P("depth", COL, ROW),
        P("depth", ROW, COL),
        P("depth", COL, ROW),
        P(ROW, COL),
        P(COL, ROW),
    )
    return jax.shard_map(
        step,
        mesh=fine,
        in_specs=placed,
        out_specs=(
            P("depth", COL, ROW),
            P(ROW, (*COL, "depth")),
            P((*COL, "depth"), ROW),
        ),
        check_vma=False,
    )
```

```python
import jax
import jax.numpy as jnp
from jax import lax
from jax.sharding import Mesh, PartitionSpec as P


root_coeff = 0.7978845608028654
cubic_coeff = 0.044715

ROW = ("yhi", "core")
COL = ("ylo", "x")
SWAP = [(0, 1), (1, 0)]


def spread(value, axis):
    copies = jnp.broadcast_to(value, (lax.axis_size(axis), *value.shape))
    return lax.all_to_all(copies, axis, split_axis=0, concat_axis=0, tiled=True)


def exchanged(value, axis):
    return lax.all_to_all(value, axis, split_axis=0, concat_axis=0, tiled=True)


def summed(pieces):
    return jnp.sum(pieces.astype(jnp.float32), axis=0)


def gelu_parts(values):
    inner = root_coeff * (values + cubic_coeff * values * values * values)
    tangent = jnp.tanh(inner)
    active = 0.5 * values * (1.0 + tangent)
    slope = 0.5 * (1.0 + tangent) + 0.5 * values * (1.0 - tangent * tangent) * root_coeff * (
        1.0 + 3.0 * cubic_coeff * values * values
    )
    return (active, slope)


def contract_last(left, right):
    return lax.dot_general(
        left, right, (((1,), (1,)), ((), ())), preferred_element_type=jnp.float32
    )


def contract_first(left, right):
    return lax.dot_general(
        left, right, (((0,), (0,)), ((), ())), preferred_element_type=jnp.float32
    )


def shifted(value, axis, by):
    length = lax.axis_size(axis)
    return lax.ppermute(value, axis, [(k, (k + by) % length) for k in range(length)])


def swapped(value):
    return lax.ppermute(value, "core", SWAP)


def block_at(blocks, index):
    return lax.dynamic_index_in_dim(blocks, index, 0, keepdims=False)


def gathered(own):
    pieces = [own] + [shifted(own, "yhi", 4 - u) for u in (1, 2, 3)]
    n = own.shape[0]
    least = jnp.array(-jnp.inf, own.dtype)
    spaced = [lax.pad(v, least, ((k * n, (3 - k) * n, 0), (0, 0, 0))) for k, v in enumerate(pieces)]
    return jnp.maximum(jnp.maximum(spaced[0], spaced[1]), jnp.maximum(spaced[2], spaced[3]))


def wide(value):
    return value.astype(jnp.float32)


def depth_parts(blocks):
    here = lax.axis_index("depth")
    pick = lambda by: block_at(blocks, (here + by) % 8)
    even = here % 2 == 0
    near_up = shifted(jnp.stack([pick(1), pick(3)]), "depth", 1)
    near_down = shifted(jnp.stack([pick(7), pick(5)]), "depth", 7)
    turns = [(k, (k + 2) % 8 if k % 2 == 0 else (k - 2) % 8) for k in range(8)]
    far = lax.ppermute(pick(4), "depth", turns)
    up = wide(pick(2)) + wide(near_up[1]) + jnp.where(even, wide(far), 0.0)
    down = wide(pick(6)) + wide(near_down[1]) + jnp.where(even, 0.0, wide(far))
    last_up = shifted(up.astype(jnp.bfloat16), "depth", 2)
    last_down = shifted(down.astype(jnp.bfloat16), "depth", 6)
    near = wide(pick(0)) + wide(near_up[0]) + wide(near_down[0])
    return near, last_up, last_down


def total(parts):
    near, last_up, last_down = parts
    return near + wide(last_up) + wide(last_down)


def step(inputs, pre_act, grad_out, weight_up, weight_down):
    core = lax.axis_index("core")
    high = lax.axis_index("yhi")
    active, slope = gelu_parts(wide(pre_act[0]))
    active, slope = lax.optimization_barrier((active.astype(jnp.bfloat16), slope))
    active_mine = gathered(active)

    both = spread(jnp.concatenate([grad_out[0], inputs[0]], axis=1), COL)
    width = inputs.shape[2]
    both = both.reshape(4, 2, *both.shape[1:])
    of = lambda c: lax.dynamic_index_in_dim(both, c, 1, keepdims=False)
    mine, other = of(core), of(1 - core)
    flat = lambda blocks: blocks.reshape(-1, blocks.shape[-1])
    away = contract_last(flat(other[..., :width]), weight_down).astype(jnp.bfloat16)
    back = swapped(away)
    kept = contract_last(flat(mine[..., :width]), weight_down)
    pair = (kept + wide(back)).astype(jnp.bfloat16).reshape(4, 64, -1)
    came = exchanged(pair, "yhi")

    active_other = swapped(active_mine)
    turned = lambda blocks: jnp.concatenate([block_at(blocks, (high + u) % 4) for u in range(4)], axis=0)
    lower_mine = lax.optimization_barrier(contract_first(active_mine, turned(mine[..., :width])))
    lower = contract_first(active_other, turned(other[..., :width])) + lower_mine
    lower = lower.astype(jnp.bfloat16)
    lower_parts = depth_parts(lower.reshape(8, -1, lower.shape[1]))

    delta_own = (sum(wide(came[k]) for k in range(4)) * slope).astype(jnp.bfloat16)
    delta_mine = flat(spread(delta_own, "yhi"))
    delta_other = swapped(delta_mine)

    upper_mine = lax.optimization_barrier(contract_first(delta_mine, flat(mine[..., width:])))
    upper = contract_first(delta_other, flat(other[..., width:])) + upper_mine
    upper = upper.astype(jnp.bfloat16)
    near, last_up, last_down = depth_parts(upper.reshape(8, -1, upper.shape[1]))

    parts_mine = contract_last(delta_mine, weight_up).astype(jnp.bfloat16)
    parts_other = contract_last(delta_other, weight_up).astype(jnp.bfloat16)
    first = jnp.where(core == 0, parts_mine, parts_other).reshape(4, 64, -1)
    second = jnp.where(core == 0, parts_other, parts_mine).reshape(4, 64, -1)
    parts = jnp.stack([first, second], axis=1).reshape(8, 64, -1)
    parts = exchanged(parts, COL)
    grad_inputs = summed(parts).astype(jnp.bfloat16)[None]
    grad_down = total(lower_parts)
    grad_inputs, grad_down, last_up = lax.optimization_barrier((grad_inputs, grad_down, last_up))
    grad_up = total((near, last_up, last_down))
    return (grad_inputs, grad_up.T, grad_down)


def solution(mesh):
    fine = Mesh(mesh.devices.reshape(4, 2, 2, 4, 8), ("yhi", "core", "ylo", "x", "depth"))
    placed = (
        P("depth", COL, ROW),
        P("depth", ROW, COL),
        P("depth", COL, ROW),
        P(ROW, COL),
        P(COL, ROW),
    )
    return jax.shard_map(
        step,
        mesh=fine,
        in_specs=placed,
        out_specs=(
            P("depth", COL, ROW),
            P(ROW, (*COL, "depth")),
            P((*COL, "depth"), ROW),
        ),
        check_vma=False,
    )
```

```python
import jax
import jax.numpy as jnp
from jax import lax
from jax.sharding import Mesh, PartitionSpec as P


root_coeff = 0.7978845608028654
cubic_coeff = 0.044715

ROW = ("yhi", "core")
COL = ("ylo", "x")
SWAP = [(0, 1), (1, 0)]


def spread(value, axis):
    copies = jnp.broadcast_to(value, (lax.axis_size(axis), *value.shape))
    return lax.all_to_all(copies, axis, split_axis=0, concat_axis=0, tiled=True)


def exchanged(value, axis):
    return lax.all_to_all(value, axis, split_axis=0, concat_axis=0, tiled=True)


def summed(pieces):
    return jnp.sum(pieces.astype(jnp.float32), axis=0)


def gelu_parts(values):
    inner = root_coeff * (values + cubic_coeff * values * values * values)
    tangent = jnp.tanh(inner)
    active = 0.5 * values * (1.0 + tangent)
    slope = 0.5 * (1.0 + tangent) + 0.5 * values * (1.0 - tangent * tangent) * root_coeff * (
        1.0 + 3.0 * cubic_coeff * values * values
    )
    return (active, slope)


def contract_last(left, right):
    return lax.dot_general(
        left, right, (((1,), (1,)), ((), ())), preferred_element_type=jnp.float32
    )


def contract_first(left, right):
    return lax.dot_general(
        left, right, (((0,), (0,)), ((), ())), preferred_element_type=jnp.float32
    )


def shifted(value, axis, by):
    length = lax.axis_size(axis)
    return lax.ppermute(value, axis, [(k, (k + by) % length) for k in range(length)])


def swapped(value):
    return lax.ppermute(value, "core", SWAP)


def block_at(blocks, index):
    return lax.dynamic_index_in_dim(blocks, index, 0, keepdims=False)


def gathered(own):
    pieces = [own] + [shifted(own, "yhi", 4 - u) for u in (1, 2, 3)]
    n = own.shape[0]
    least = jnp.array(-jnp.inf, own.dtype)
    spaced = [lax.pad(v, least, ((k * n, (3 - k) * n, 0), (0, 0, 0))) for k, v in enumerate(pieces)]
    return jnp.maximum(jnp.maximum(spaced[0], spaced[1]), jnp.maximum(spaced[2], spaced[3]))


def wide(value):
    return value.astype(jnp.float32)


def depth_parts(blocks, straight):
    here = lax.axis_index("depth")
    pick = lambda by: block_at(blocks, (here + by) % 8)
    even = here % 2 == 0
    near_up = shifted(jnp.stack([pick(1), pick(3)]), "depth", 1)
    near_down = shifted(jnp.stack([pick(7), pick(5)]), "depth", 7)
    up = wide(pick(2)) + wide(near_up[1])
    down = wide(pick(6)) + wide(near_down[1])
    if straight:
        far = [shifted(pick(4), "depth", 4)]
    else:
        turns = [(k, (k + 2) % 8 if k % 2 == 0 else (k - 2) % 8) for k in range(8)]
        turn = wide(lax.ppermute(pick(4), "depth", turns))
        up, down, far = up + jnp.where(even, turn, 0.0), down + jnp.where(even, 0.0, turn), []
    last_up = shifted(up.astype(jnp.bfloat16), "depth", 2)
    last_down = shifted(down.astype(jnp.bfloat16), "depth", 6)
    near = wide(pick(0)) + wide(near_up[0]) + wide(near_down[0])
    return near, last_up, last_down, *far


def total(parts):
    return sum(wide(part) for part in parts)


def step(inputs, pre_act, grad_out, weight_up, weight_down):
    core = lax.axis_index("core")
    high = lax.axis_index("yhi")
    active, slope = gelu_parts(wide(pre_act[0]))
    active, slope = lax.optimization_barrier((active.astype(jnp.bfloat16), slope))
    active_mine = gathered(active)

    both = spread(jnp.concatenate([grad_out[0], inputs[0]], axis=1), COL)
    width = inputs.shape[2]
    both = both.reshape(4, 2, *both.shape[1:])
    of = lambda c: lax.dynamic_index_in_dim(both, c, 1, keepdims=False)
    mine, other = of(core), of(1 - core)
    flat = lambda blocks: blocks.reshape(-1, blocks.shape[-1])
    away = contract_last(flat(other[..., :width]), weight_down).astype(jnp.bfloat16)
    back = swapped(away)
    kept = contract_last(flat(mine[..., :width]), weight_down)
    pair = (kept + wide(back)).astype(jnp.bfloat16).reshape(4, 64, -1)
    came = exchanged(pair, "yhi")

    active_other = swapped(active_mine)
    turned = lambda blocks: jnp.concatenate([block_at(blocks, (high + u) % 4) for u in range(4)], axis=0)
    lower_mine = lax.optimization_barrier(contract_first(active_mine, turned(mine[..., :width])))
    lower = contract_first(active_other, turned(other[..., :width])) + lower_mine
    lower = lower.astype(jnp.bfloat16)
    lower_parts = depth_parts(lower.reshape(8, -1, lower.shape[1]), True)

    delta_own = (sum(wide(came[k]) for k in range(4)) * slope).astype(jnp.bfloat16)
    delta_mine = flat(spread(delta_own, "yhi"))
    delta_other = swapped(delta_mine)

    upper_mine = lax.optimization_barrier(contract_first(delta_mine, flat(mine[..., width:])))
    upper = contract_first(delta_other, flat(other[..., width:])) + upper_mine
    upper = upper.astype(jnp.bfloat16)
    near, last_up, last_down = depth_parts(upper.reshape(8, -1, upper.shape[1]), False)

    parts_mine = contract_last(delta_mine, weight_up).astype(jnp.bfloat16)
    parts_other = contract_last(delta_other, weight_up).astype(jnp.bfloat16)
    first = jnp.where(core == 0, parts_mine, parts_other).reshape(4, 64, -1)
    second = jnp.where(core == 0, parts_other, parts_mine).reshape(4, 64, -1)
    parts = jnp.stack([first, second], axis=1).reshape(8, 64, -1)
    parts = exchanged(parts, COL)
    grad_inputs = summed(parts).astype(jnp.bfloat16)[None]
    grad_down = total(lower_parts)
    grad_inputs, grad_down, last_up = lax.optimization_barrier((grad_inputs, grad_down, last_up))
    grad_up = total((near, last_up, last_down))
    return (grad_inputs, grad_up.T, grad_down)


def solution(mesh):
    fine = Mesh(mesh.devices.reshape(4, 2, 2, 4, 8), ("yhi", "core", "ylo", "x", "depth"))
    placed = (
        P("depth", COL, ROW),
        P("depth", ROW, COL),
        P("depth", COL, ROW),
        P(ROW, COL),
        P(COL, ROW),
    )
    return jax.shard_map(
        step,
        mesh=fine,
        in_specs=placed,
        out_specs=(
            P("depth", COL, ROW),
            P(ROW, (*COL, "depth")),
            P((*COL, "depth"), ROW),
        ),
        check_vma=False,
    )
```

```python
import jax
import jax.numpy as jnp
from jax import lax
from jax.sharding import Mesh, PartitionSpec as P


root_coeff = 0.7978845608028654
cubic_coeff = 0.044715

ROW = ("yhi", "core")
COL = ("ylo", "x")
SWAP = [(0, 1), (1, 0)]


def spread(value, axis):
    copies = jnp.broadcast_to(value, (lax.axis_size(axis), *value.shape))
    return lax.all_to_all(copies, axis, split_axis=0, concat_axis=0, tiled=True)


def exchanged(value, axis):
    return lax.all_to_all(value, axis, split_axis=0, concat_axis=0, tiled=True)


def summed(pieces):
    return jnp.sum(pieces.astype(jnp.float32), axis=0)


def gelu_parts(values):
    inner = root_coeff * (values + cubic_coeff * values * values * values)
    tangent = jnp.tanh(inner)
    active = 0.5 * values * (1.0 + tangent)
    slope = 0.5 * (1.0 + tangent) + 0.5 * values * (1.0 - tangent * tangent) * root_coeff * (
        1.0 + 3.0 * cubic_coeff * values * values
    )
    return (active, slope)


def contract_last(left, right):
    return lax.dot_general(
        left, right, (((1,), (1,)), ((), ())), preferred_element_type=jnp.float32
    )


def contract_first(left, right):
    return lax.dot_general(
        left, right, (((0,), (0,)), ((), ())), preferred_element_type=jnp.float32
    )


def shifted(value, axis, by):
    length = lax.axis_size(axis)
    return lax.ppermute(value, axis, [(k, (k + by) % length) for k in range(length)])


def swapped(value):
    return lax.ppermute(value, "core", SWAP)


def block_at(blocks, index):
    return lax.dynamic_index_in_dim(blocks, index, 0, keepdims=False)


def gathered(own):
    after, before = shifted(own, "yhi", 3), shifted(own, "yhi", 1)
    across = shifted(own, "yhi", 2)
    n = own.shape[0]
    least = jnp.array(-jnp.inf, own.dtype)
    pieces = enumerate((own, after, across, before))
    spaced = [lax.pad(v, least, ((k * n, (3 - k) * n, 0), (0, 0, 0))) for k, v in pieces]
    return jnp.maximum(jnp.maximum(spaced[0], spaced[1]), jnp.maximum(spaced[2], spaced[3]))


def wide(value):
    return value.astype(jnp.float32)


def depth_parts(blocks):
    here = lax.axis_index("depth")
    pick = lambda by: block_at(blocks, (here + by) % 8)
    near_up = shifted(jnp.stack([pick(1), pick(3)]), "depth", 1)
    near_down = shifted(jnp.stack([pick(7), pick(5)]), "depth", 7)
    far = shifted(pick(4), "depth", 4)
    up = wide(pick(2)) + wide(near_up[1])
    down = wide(pick(6)) + wide(near_down[1])
    last_up = shifted(up.astype(jnp.bfloat16), "depth", 2)
    last_down = shifted(down.astype(jnp.bfloat16), "depth", 6)
    near = wide(pick(0)) + wide(near_up[0]) + wide(near_down[0])
    return near, last_up, last_down, far


def total(parts):
    return sum(wide(part) for part in parts)


def step(inputs, pre_act, grad_out, weight_up, weight_down):
    core = lax.axis_index("core")
    high = lax.axis_index("yhi")
    active, slope = gelu_parts(wide(pre_act[0]))
    active, slope = lax.optimization_barrier((active.astype(jnp.bfloat16), slope))
    active_mine = gathered(active)

    both = spread(jnp.concatenate([grad_out[0], inputs[0]], axis=1), COL)
    width = inputs.shape[2]
    both = both.reshape(4, 2, *both.shape[1:])
    of = lambda c: lax.dynamic_index_in_dim(both, c, 1, keepdims=False)
    mine, other = of(core), of(1 - core)
    flat = lambda blocks: blocks.reshape(-1, blocks.shape[-1])
    away = contract_last(flat(other[..., :width]), weight_down).astype(jnp.bfloat16)
    back = swapped(away)
    kept = contract_last(flat(mine[..., :width]), weight_down)
    pair = (kept + wide(back)).astype(jnp.bfloat16).reshape(4, 64, -1)
    came = exchanged(pair, "yhi")

    active_other = swapped(active_mine)
    turned = lambda blocks: jnp.concatenate([block_at(blocks, (high + u) % 4) for u in range(4)], axis=0)
    lower_mine = lax.optimization_barrier(contract_first(active_mine, turned(mine[..., :width])))
    lower = contract_first(active_other, turned(other[..., :width])) + lower_mine
    lower = lower.astype(jnp.bfloat16)
    lower_parts = depth_parts(lower.reshape(8, -1, lower.shape[1]))

    delta_own = (sum(wide(came[k]) for k in range(4)) * slope).astype(jnp.bfloat16)
    delta_mine = flat(spread(delta_own, "yhi"))
    delta_other = swapped(delta_mine)

    upper_mine = lax.optimization_barrier(contract_first(delta_mine, flat(mine[..., width:])))
    upper = contract_first(delta_other, flat(other[..., width:])) + upper_mine
    upper = upper.astype(jnp.bfloat16)
    near, last_up, *rest = depth_parts(upper.reshape(8, -1, upper.shape[1]))

    parts_mine = contract_last(delta_mine, weight_up).astype(jnp.bfloat16)
    parts_other = contract_last(delta_other, weight_up).astype(jnp.bfloat16)
    first = jnp.where(core == 0, parts_mine, parts_other).reshape(4, 64, -1)
    second = jnp.where(core == 0, parts_other, parts_mine).reshape(4, 64, -1)
    parts = jnp.stack([first, second], axis=1).reshape(8, 64, -1)
    parts = exchanged(parts, COL)
    grad_inputs = summed(parts).astype(jnp.bfloat16)[None]
    grad_down = total(lower_parts)
    grad_inputs, grad_down, last_up = lax.optimization_barrier((grad_inputs, grad_down, last_up))
    grad_up = total((near, last_up, *rest))
    return (grad_inputs, grad_up.T, grad_down)


def solution(mesh):
    fine = Mesh(mesh.devices.reshape(4, 2, 2, 4, 8), ("yhi", "core", "ylo", "x", "depth"))
    placed = (
        P("depth", COL, ROW),
        P("depth", ROW, COL),
        P("depth", COL, ROW),
        P(ROW, COL),
        P(COL, ROW),
    )
    return jax.shard_map(
        step,
        mesh=fine,
        in_specs=placed,
        out_specs=(
            P("depth", COL, ROW),
            P(ROW, (*COL, "depth")),
            P((*COL, "depth"), ROW),
        ),
        check_vma=False,
    )
```

```python
import jax
import jax.numpy as jnp
from jax import lax
from jax.sharding import Mesh, PartitionSpec as P


root_coeff = 0.7978845608028654
cubic_coeff = 0.044715

ROW = ("yhi", "core")
COL = ("ylo", "x")
SWAP = [(0, 1), (1, 0)]


def spread(value, axis):
    copies = jnp.broadcast_to(value, (lax.axis_size(axis), *value.shape))
    return lax.all_to_all(copies, axis, split_axis=0, concat_axis=0, tiled=True)


def exchanged(value, axis):
    return lax.all_to_all(value, axis, split_axis=0, concat_axis=0, tiled=True)


def summed(pieces):
    return jnp.sum(pieces.astype(jnp.float32), axis=0)


def gelu_parts(values):
    inner = root_coeff * (values + cubic_coeff * values * values * values)
    tangent = jnp.tanh(inner)
    active = 0.5 * values * (1.0 + tangent)
    slope = 0.5 * (1.0 + tangent) + 0.5 * values * (1.0 - tangent * tangent) * root_coeff * (
        1.0 + 3.0 * cubic_coeff * values * values
    )
    return (active, slope)


def contract_last(left, right):
    return lax.dot_general(
        left, right, (((1,), (1,)), ((), ())), preferred_element_type=jnp.float32
    )


def contract_first(left, right):
    return lax.dot_general(
        left, right, (((0,), (0,)), ((), ())), preferred_element_type=jnp.float32
    )


def shifted(value, axis, by):
    length = lax.axis_size(axis)
    return lax.ppermute(value, axis, [(k, (k + by) % length) for k in range(length)])


def swapped(value):
    return lax.ppermute(value, "core", SWAP)


def block_at(blocks, index):
    return lax.dynamic_index_in_dim(blocks, index, 0, keepdims=False)


def gathered(own):
    pieces = [own] + [shifted(own, "yhi", 4 - u) for u in (1, 2, 3)]
    n = own.shape[0]
    least = jnp.array(-jnp.inf, own.dtype)
    spaced = [lax.pad(v, least, ((k * n, (3 - k) * n, 0), (0, 0, 0))) for k, v in enumerate(pieces)]
    return jnp.maximum(jnp.maximum(spaced[0], spaced[1]), jnp.maximum(spaced[2], spaced[3]))


def wide(value):
    return value.astype(jnp.float32)


def depth_parts(blocks, straight):
    here = lax.axis_index("depth")
    pick = lambda by: block_at(blocks, (here + by) % 8)
    even = here % 2 == 0
    near_up = shifted(jnp.stack([pick(1), pick(3)]), "depth", 1)
    near_down = shifted(jnp.stack([pick(7), pick(5)]), "depth", 7)
    up = wide(pick(2)) + wide(near_up[1])
    down = wide(pick(6)) + wide(near_down[1])
    if straight:
        far = [shifted(pick(4), "depth", 4)]
    else:
        turns = [(k, (k + 2) % 8 if k % 2 == 0 else (k - 2) % 8) for k in range(8)]
        turn = wide(lax.ppermute(pick(4), "depth", turns))
        up, down, far = up + jnp.where(even, turn, 0.0), down + jnp.where(even, 0.0, turn), []
    last_up = shifted(up.astype(jnp.bfloat16), "depth", 2)
    last_down = shifted(down.astype(jnp.bfloat16), "depth", 6)
    near = wide(pick(0)) + wide(near_up[0]) + wide(near_down[0])
    return near, last_up, last_down, *far


def total(parts):
    return sum(wide(part) for part in parts)


def step(inputs, pre_act, grad_out, weight_up, weight_down):
    core = lax.axis_index("core")
    high = lax.axis_index("yhi")
    active, slope = gelu_parts(wide(pre_act[0]))
    active, slope = lax.optimization_barrier((active.astype(jnp.bfloat16), slope))
    active_mine = gathered(active)

    by_core = lambda blocks: blocks.reshape(4, 2, *blocks.shape[1:])
    of = lambda blocks, c: lax.dynamic_index_in_dim(blocks, c, 1, keepdims=False)
    flat = lambda blocks: blocks.reshape(-1, blocks.shape[-1])
    layer_grads = by_core(spread(grad_out[0], COL))
    layer_inputs = by_core(spread(inputs[0], COL))
    grads_mine, grads_other = of(layer_grads, core), of(layer_grads, 1 - core)
    away = contract_last(flat(grads_other), weight_down).astype(jnp.bfloat16)
    back = swapped(away)
    kept = contract_last(flat(grads_mine), weight_down)
    pair = (kept + wide(back)).astype(jnp.bfloat16).reshape(4, 64, -1)
    came = exchanged(pair, "yhi")
    layer_inputs, _ = lax.optimization_barrier((layer_inputs, pair))
    inputs_mine, inputs_other = of(layer_inputs, core), of(layer_inputs, 1 - core)

    active_other = swapped(active_mine)
    turned = lambda blocks: jnp.concatenate([block_at(blocks, (high + u) % 4) for u in range(4)], axis=0)
    lower_mine = lax.optimization_barrier(contract_first(active_mine, turned(grads_mine)))
    lower = contract_first(active_other, turned(grads_other)) + lower_mine
    lower = lower.astype(jnp.bfloat16)
    lower_parts = depth_parts(lower.reshape(8, -1, lower.shape[1]), True)

    delta_own = (sum(wide(came[k]) for k in range(4)) * slope).astype(jnp.bfloat16)
    delta_mine = flat(spread(delta_own, "yhi"))
    delta_other = swapped(delta_mine)

    upper_mine = lax.optimization_barrier(contract_first(delta_mine, flat(inputs_mine)))
    upper = contract_first(delta_other, flat(inputs_other)) + upper_mine
    upper = upper.astype(jnp.bfloat16)
    near, last_up, last_down = depth_parts(upper.reshape(8, -1, upper.shape[1]), False)

    parts_mine = contract_last(delta_mine, weight_up).astype(jnp.bfloat16)
    parts_other = contract_last(delta_other, weight_up).astype(jnp.bfloat16)
    first = jnp.where(core == 0, parts_mine, parts_other).reshape(4, 64, -1)
    second = jnp.where(core == 0, parts_other, parts_mine).reshape(4, 64, -1)
    parts = jnp.stack([first, second], axis=1).reshape(8, 64, -1)
    parts = exchanged(parts, COL)
    grad_inputs = summed(parts).astype(jnp.bfloat16)[None]
    grad_down = total(lower_parts)
    grad_inputs, grad_down, last_up = lax.optimization_barrier((grad_inputs, grad_down, last_up))
    grad_up = total((near, last_up, last_down))
    return (grad_inputs, grad_up.T, grad_down)


def solution(mesh):
    fine = Mesh(mesh.devices.reshape(4, 2, 2, 4, 8), ("yhi", "core", "ylo", "x", "depth"))
    placed = (
        P("depth", COL, ROW),
        P("depth", ROW, COL),
        P("depth", COL, ROW),
        P(ROW, COL),
        P(COL, ROW),
    )
    return jax.shard_map(
        step,
        mesh=fine,
        in_specs=placed,
        out_specs=(
            P("depth", COL, ROW),
            P(ROW, (*COL, "depth")),
            P((*COL, "depth"), ROW),
        ),
        check_vma=False,
    )
```

```python
import jax
import jax.numpy as jnp
from jax import lax
from jax.experimental import pallas as pl
from jax.experimental.pallas import tpu as pltpu
from jax.sharding import Mesh, PartitionSpec as P


root_coeff = 0.7978845608028654
cubic_coeff = 0.044715

ROW = ("yhi", "core")
COL = ("ylo", "x")
SWAP = [(0, 1), (1, 0)]


def spread(value, axis):
    copies = jnp.broadcast_to(value, (lax.axis_size(axis), *value.shape))
    return lax.all_to_all(copies, axis, split_axis=0, concat_axis=0, tiled=True)


def exchanged(value, axis):
    return lax.all_to_all(value, axis, split_axis=0, concat_axis=0, tiled=True)


def summed(pieces):
    return jnp.sum(pieces.astype(jnp.float32), axis=0)


def gelu_parts(values):
    inner = root_coeff * (values + cubic_coeff * values * values * values)
    tangent = jnp.tanh(inner)
    active = 0.5 * values * (1.0 + tangent)
    slope = 0.5 * (1.0 + tangent) + 0.5 * values * (1.0 - tangent * tangent) * root_coeff * (
        1.0 + 3.0 * cubic_coeff * values * values
    )
    return (active, slope)


def contract_last(left, right):
    return lax.dot_general(
        left, right, (((1,), (1,)), ((), ())), preferred_element_type=jnp.float32
    )


def contract_first(left, right):
    return lax.dot_general(
        left, right, (((0,), (0,)), ((), ())), preferred_element_type=jnp.float32
    )


def shifted(value, axis, by):
    length = lax.axis_size(axis)
    return lax.ppermute(value, axis, [(k, (k + by) % length) for k in range(length)])


def swapped(value):
    return lax.ppermute(value, "core", SWAP)


def block_at(blocks, index):
    return lax.dynamic_index_in_dim(blocks, index, 0, keepdims=False)


def gathered(own):
    pieces = [own] + [shifted(own, "yhi", 4 - u) for u in (1, 2, 3)]
    n = own.shape[0]
    least = jnp.array(-jnp.inf, own.dtype)
    spaced = [lax.pad(v, least, ((k * n, (3 - k) * n, 0), (0, 0, 0))) for k, v in enumerate(pieces)]
    return jnp.maximum(jnp.maximum(spaced[0], spaced[1]), jnp.maximum(spaced[2], spaced[3]))


def wide(value):
    return value.astype(jnp.float32)


def onward_kernel(spot, own_up, own_down, near_up, near_down, *rest):
    *turn, up, down = rest
    upward = wide(own_up[0]) + wide(near_up[0])
    downward = wide(own_down[0]) + wide(near_down[0])
    if turn:
        came = wide(turn[0][...])
        upward = upward + jnp.where(spot[2] == 1, came, 0.0)
        downward = downward + jnp.where(spot[2] == 1, 0.0, came)
    up[...] = upward.astype(up.dtype)
    down[...] = downward.astype(down.dtype)


def onward(blocks, near_up, near_down, *turn):
    here = lax.axis_index("depth")
    spot = jnp.stack([(here + 2) % 8, (here + 6) % 8, 1 - here % 2]).astype(jnp.int32)
    shape = blocks.shape[1:]
    block = lambda pick: pl.BlockSpec((1, *shape), pick)
    specs = [block(lambda i, s: (s[0], 0, 0)), block(lambda i, s: (s[1], 0, 0))]
    specs += [block(lambda i, s: (1, 0, 0))] * 2 + [pl.BlockSpec(shape, lambda i, s: (0, 0))] * len(turn)
    whole = pl.BlockSpec(memory_space=pltpu.VMEM)
    return pl.pallas_call(
        onward_kernel,
        out_shape=[pltpu.VMEM(shape, blocks.dtype)] * 2,
        grid_spec=pltpu.PrefetchScalarGridSpec(
            num_scalar_prefetch=1, grid=(1,), in_specs=specs, out_specs=[whole] * 2
        ),
        name="onward",
    )(spot, blocks, blocks, near_up, near_down, *turn)


def depth_parts(blocks, straight):
    here = lax.axis_index("depth")
    pick = lambda by: block_at(blocks, (here + by) % 8)
    near_up = shifted(jnp.stack([pick(1), pick(3)]), "depth", 1)
    near_down = shifted(jnp.stack([pick(7), pick(5)]), "depth", 7)
    if straight:
        far, turn = [shifted(pick(4), "depth", 4)], []
    else:
        turns = [(k, (k + 2) % 8 if k % 2 == 0 else (k - 2) % 8) for k in range(8)]
        far, turn = [], [lax.ppermute(pick(4), "depth", turns)]
    up, down = onward(blocks, near_up, near_down, *turn)
    last_up = shifted(up, "depth", 2)
    last_down = shifted(down, "depth", 6)
    near = wide(pick(0)) + wide(near_up[0]) + wide(near_down[0])
    return near, last_up, last_down, *far


def total(parts):
    return sum(wide(part) for part in parts)


def step(inputs, pre_act, grad_out, weight_up, weight_down):
    core = lax.axis_index("core")
    high = lax.axis_index("yhi")
    active, slope = gelu_parts(wide(pre_act[0]))
    active, slope = lax.optimization_barrier((active.astype(jnp.bfloat16), slope))
    active_mine = gathered(active)

    both = spread(jnp.concatenate([grad_out[0], inputs[0]], axis=1), COL)
    width = inputs.shape[2]
    both = both.reshape(4, 2, *both.shape[1:])
    of = lambda c: lax.dynamic_index_in_dim(both, c, 1, keepdims=False)
    mine, other = of(core), of(1 - core)
    flat = lambda blocks: blocks.reshape(-1, blocks.shape[-1])
    away = contract_last(flat(other[..., :width]), weight_down).astype(jnp.bfloat16)
    back = swapped(away)
    kept = contract_last(flat(mine[..., :width]), weight_down)
    pair = (kept + wide(back)).astype(jnp.bfloat16).reshape(4, 64, -1)
    came = exchanged(pair, "yhi")

    active_other = swapped(active_mine)
    turned = lambda blocks: jnp.concatenate([block_at(blocks, (high + u) % 4) for u in range(4)], axis=0)
    lower_mine = lax.optimization_barrier(contract_first(active_mine, turned(mine[..., :width])))
    lower = contract_first(active_other, turned(other[..., :width])) + lower_mine
    lower = lower.astype(jnp.bfloat16)
    lower_parts = depth_parts(lower.reshape(8, -1, lower.shape[1]), True)

    delta_own = (sum(wide(came[k]) for k in range(4)) * slope).astype(jnp.bfloat16)
    delta_mine = flat(spread(delta_own, "yhi"))
    delta_other = swapped(delta_mine)

    upper_mine = lax.optimization_barrier(contract_first(delta_mine, flat(mine[..., width:])))
    upper = contract_first(delta_other, flat(other[..., width:])) + upper_mine
    upper = upper.astype(jnp.bfloat16)
    near, last_up, last_down = depth_parts(upper.reshape(8, -1, upper.shape[1]), False)

    parts_mine = contract_last(delta_mine, weight_up).astype(jnp.bfloat16)
    parts_other = contract_last(delta_other, weight_up).astype(jnp.bfloat16)
    first = jnp.where(core == 0, parts_mine, parts_other).reshape(4, 64, -1)
    second = jnp.where(core == 0, parts_other, parts_mine).reshape(4, 64, -1)
    parts = jnp.stack([first, second], axis=1).reshape(8, 64, -1)
    parts = exchanged(parts, COL)
    grad_inputs = summed(parts).astype(jnp.bfloat16)[None]
    grad_down = total(lower_parts)
    grad_inputs, grad_down, last_up = lax.optimization_barrier((grad_inputs, grad_down, last_up))
    grad_up = total((near, last_up, last_down))
    return (grad_inputs, grad_up.T, grad_down)


def solution(mesh):
    fine = Mesh(mesh.devices.reshape(4, 2, 2, 4, 8), ("yhi", "core", "ylo", "x", "depth"))
    placed = (
        P("depth", COL, ROW),
        P("depth", ROW, COL),
        P("depth", COL, ROW),
        P(ROW, COL),
        P(COL, ROW),
    )
    return jax.shard_map(
        step,
        mesh=fine,
        in_specs=placed,
        out_specs=(
            P("depth", COL, ROW),
            P(ROW, (*COL, "depth")),
            P((*COL, "depth"), ROW),
        ),
        check_vma=False,
    )
```

```python
import jax
import jax.numpy as jnp
from jax import lax
from jax.experimental import pallas as pl
from jax.experimental.pallas import tpu as pltpu
from jax.sharding import Mesh, PartitionSpec as P


root_coeff = 0.7978845608028654
cubic_coeff = 0.044715

ROW = ("yhi", "core")
COL = ("ylo", "x")
SWAP = [(0, 1), (1, 0)]


def spread(value, axis):
    copies = jnp.broadcast_to(value, (lax.axis_size(axis), *value.shape))
    return lax.all_to_all(copies, axis, split_axis=0, concat_axis=0, tiled=True)


def exchanged(value, axis):
    return lax.all_to_all(value, axis, split_axis=0, concat_axis=0, tiled=True)


def summed(pieces):
    return jnp.sum(pieces.astype(jnp.float32), axis=0)


def gelu_parts(values):
    inner = root_coeff * (values + cubic_coeff * values * values * values)
    tangent = jnp.tanh(inner)
    active = 0.5 * values * (1.0 + tangent)
    slope = 0.5 * (1.0 + tangent) + 0.5 * values * (1.0 - tangent * tangent) * root_coeff * (
        1.0 + 3.0 * cubic_coeff * values * values
    )
    return (active, slope)


def contract_last(left, right):
    return lax.dot_general(
        left, right, (((1,), (1,)), ((), ())), preferred_element_type=jnp.float32
    )


def contract_first(left, right):
    return lax.dot_general(
        left, right, (((0,), (0,)), ((), ())), preferred_element_type=jnp.float32
    )


def shifted(value, axis, by):
    length = lax.axis_size(axis)
    return lax.ppermute(value, axis, [(k, (k + by) % length) for k in range(length)])


def swapped(value):
    return lax.ppermute(value, "core", SWAP)


def block_at(blocks, index):
    return lax.dynamic_index_in_dim(blocks, index, 0, keepdims=False)


def gathered(own):
    pieces = [own] + [shifted(own, "yhi", 4 - u) for u in (1, 2, 3)]
    n = own.shape[0]
    least = jnp.array(-jnp.inf, own.dtype)
    spaced = [lax.pad(v, least, ((k * n, (3 - k) * n, 0), (0, 0, 0))) for k, v in enumerate(pieces)]
    return jnp.maximum(jnp.maximum(spaced[0], spaced[1]), jnp.maximum(spaced[2], spaced[3]))


def wide(value):
    return value.astype(jnp.float32)


def onward_kernel(spot, own_up, own_down, near_up, near_down, *rest):
    *turn, up, down = rest
    upward = wide(own_up[0]) + wide(near_up[0])
    downward = wide(own_down[0]) + wide(near_down[0])
    if turn:
        came = wide(turn[0][...])
        upward = upward + jnp.where(spot[2] == 1, came, 0.0)
        downward = downward + jnp.where(spot[2] == 1, 0.0, came)
    up[...] = upward.astype(up.dtype)
    down[...] = downward.astype(down.dtype)


def onward(blocks, near_up, near_down, *turn):
    here = lax.axis_index("depth")
    spot = jnp.stack([(here + 2) % 8, (here + 6) % 8, 1 - here % 2]).astype(jnp.int32)
    shape = blocks.shape[1:]
    block = lambda pick: pl.BlockSpec((1, *shape), pick)
    specs = [block(lambda i, s: (s[0], 0, 0)), block(lambda i, s: (s[1], 0, 0))]
    specs += [block(lambda i, s: (1, 0, 0))] * 2 + [pl.BlockSpec(shape, lambda i, s: (0, 0))] * len(turn)
    whole = pl.BlockSpec(memory_space=pltpu.VMEM)
    return pl.pallas_call(
        onward_kernel,
        out_shape=[pltpu.VMEM(shape, blocks.dtype)] * 2,
        grid_spec=pltpu.PrefetchScalarGridSpec(
            num_scalar_prefetch=1, grid=(1,), in_specs=specs, out_specs=[whole] * 2
        ),
        name="onward",
    )(spot, blocks, blocks, near_up, near_down, *turn)


def leaving_kernel(spot, first, third, seventh, fifth, fourth, to_up, to_down, across):
    to_up[0] = first[0]
    to_up[1] = third[0]
    to_down[0] = seventh[0]
    to_down[1] = fifth[0]
    across[...] = fourth[0]


def leaving(blocks):
    here = lax.axis_index("depth")
    spot = jnp.stack([(here + by) % 8 for by in (1, 3, 7, 5, 4)]).astype(jnp.int32)
    shape = blocks.shape[1:]
    specs = [pl.BlockSpec((1, *shape), lambda i, s, k=k: (s[k], 0, 0)) for k in range(5)]
    whole = pl.BlockSpec(memory_space=pltpu.VMEM)
    pair = pltpu.VMEM((2, *shape), blocks.dtype)
    return pl.pallas_call(
        leaving_kernel,
        out_shape=[pair, pair, pltpu.VMEM(shape, blocks.dtype)],
        grid_spec=pltpu.PrefetchScalarGridSpec(
            num_scalar_prefetch=1, grid=(1,), in_specs=specs, out_specs=[whole] * 3
        ),
        name="leaving",
    )(spot, *[blocks] * 5)


def depth_parts(blocks, straight):
    here = lax.axis_index("depth")
    pick = lambda by: block_at(blocks, (here + by) % 8)
    if straight:
        to_up, to_down = jnp.stack([pick(1), pick(3)]), jnp.stack([pick(7), pick(5)])
        across = pick(4)
    else:
        to_up, to_down, across = leaving(blocks)
    near_up = shifted(to_up, "depth", 1)
    near_down = shifted(to_down, "depth", 7)
    if straight:
        far, turn = [shifted(across, "depth", 4)], []
    else:
        turns = [(k, (k + 2) % 8 if k % 2 == 0 else (k - 2) % 8) for k in range(8)]
        far, turn = [], [lax.ppermute(across, "depth", turns)]
    up, down = onward(blocks, near_up, near_down, *turn)
    last_up = shifted(up, "depth", 2)
    last_down = shifted(down, "depth", 6)
    near = wide(pick(0)) + wide(near_up[0]) + wide(near_down[0])
    return near, last_up, last_down, *far


def total(parts):
    return sum(wide(part) for part in parts)


def step(inputs, pre_act, grad_out, weight_up, weight_down):
    core = lax.axis_index("core")
    high = lax.axis_index("yhi")
    active, slope = gelu_parts(wide(pre_act[0]))
    active, slope = lax.optimization_barrier((active.astype(jnp.bfloat16), slope))
    active_mine = gathered(active)

    both = spread(jnp.concatenate([grad_out[0], inputs[0]], axis=1), COL)
    width = inputs.shape[2]
    both = both.reshape(4, 2, *both.shape[1:])
    of = lambda c: lax.dynamic_index_in_dim(both, c, 1, keepdims=False)
    mine, other = of(core), of(1 - core)
    flat = lambda blocks: blocks.reshape(-1, blocks.shape[-1])
    away = contract_last(flat(other[..., :width]), weight_down).astype(jnp.bfloat16)
    back = swapped(away)
    kept = contract_last(flat(mine[..., :width]), weight_down)
    pair = (kept + wide(back)).astype(jnp.bfloat16).reshape(4, 64, -1)
    came = exchanged(pair, "yhi")

    active_other = swapped(active_mine)
    turned = lambda blocks: jnp.concatenate([block_at(blocks, (high + u) % 4) for u in range(4)], axis=0)
    lower_mine = lax.optimization_barrier(contract_first(active_mine, turned(mine[..., :width])))
    lower = contract_first(active_other, turned(other[..., :width])) + lower_mine
    lower = lower.astype(jnp.bfloat16)
    lower_parts = depth_parts(lower.reshape(8, -1, lower.shape[1]), True)

    delta_own = (sum(wide(came[k]) for k in range(4)) * slope).astype(jnp.bfloat16)
    delta_mine = flat(spread(delta_own, "yhi"))
    delta_other = swapped(delta_mine)

    upper_mine = lax.optimization_barrier(contract_first(delta_mine, flat(mine[..., width:])))
    upper = contract_first(delta_other, flat(other[..., width:])) + upper_mine
    upper = upper.astype(jnp.bfloat16)
    near, last_up, last_down = depth_parts(upper.reshape(8, -1, upper.shape[1]), False)

    parts_mine = contract_last(delta_mine, weight_up).astype(jnp.bfloat16)
    parts_other = contract_last(delta_other, weight_up).astype(jnp.bfloat16)
    first = jnp.where(core == 0, parts_mine, parts_other).reshape(4, 64, -1)
    second = jnp.where(core == 0, parts_other, parts_mine).reshape(4, 64, -1)
    parts = jnp.stack([first, second], axis=1).reshape(8, 64, -1)
    parts = exchanged(parts, COL)
    grad_inputs = summed(parts).astype(jnp.bfloat16)[None]
    grad_down = total(lower_parts)
    grad_inputs, grad_down, last_up = lax.optimization_barrier((grad_inputs, grad_down, last_up))
    grad_up = total((near, last_up, last_down))
    return (grad_inputs, grad_up.T, grad_down)


def solution(mesh):
    fine = Mesh(mesh.devices.reshape(4, 2, 2, 4, 8), ("yhi", "core", "ylo", "x", "depth"))
    placed = (
        P("depth", COL, ROW),
        P("depth", ROW, COL),
        P("depth", COL, ROW),
        P(ROW, COL),
        P(COL, ROW),
    )
    return jax.shard_map(
        step,
        mesh=fine,
        in_specs=placed,
        out_specs=(
            P("depth", COL, ROW),
            P(ROW, (*COL, "depth")),
            P((*COL, "depth"), ROW),
        ),
        check_vma=False,
    )
```

```python
import jax
import jax.numpy as jnp
from jax import lax
from jax.experimental import pallas as pl
from jax.experimental.pallas import tpu as pltpu
from jax.sharding import Mesh, PartitionSpec as P


root_coeff = 0.7978845608028654
cubic_coeff = 0.044715

ROW = ("yhi", "core")
COL = ("ylo", "x")
SWAP = [(0, 1), (1, 0)]


def spread(value, axis):
    copies = jnp.broadcast_to(value, (lax.axis_size(axis), *value.shape))
    return lax.all_to_all(copies, axis, split_axis=0, concat_axis=0, tiled=True)


def exchanged(value, axis):
    return lax.all_to_all(value, axis, split_axis=0, concat_axis=0, tiled=True)


def summed(pieces):
    return jnp.sum(pieces.astype(jnp.float32), axis=0)


def gelu_parts(values):
    inner = root_coeff * (values + cubic_coeff * values * values * values)
    tangent = jnp.tanh(inner)
    active = 0.5 * values * (1.0 + tangent)
    slope = 0.5 * (1.0 + tangent) + 0.5 * values * (1.0 - tangent * tangent) * root_coeff * (
        1.0 + 3.0 * cubic_coeff * values * values
    )
    return (active, slope)


def contract_last(left, right):
    return lax.dot_general(
        left, right, (((1,), (1,)), ((), ())), preferred_element_type=jnp.float32
    )


def contract_first(left, right):
    return lax.dot_general(
        left, right, (((0,), (0,)), ((), ())), preferred_element_type=jnp.float32
    )


def shifted(value, axis, by):
    length = lax.axis_size(axis)
    return lax.ppermute(value, axis, [(k, (k + by) % length) for k in range(length)])


def swapped(value):
    return lax.ppermute(value, "core", SWAP)


def block_at(blocks, index):
    return lax.dynamic_index_in_dim(blocks, index, 0, keepdims=False)


def gathered(own):
    pieces = [own] + [shifted(own, "yhi", 4 - u) for u in (1, 2, 3)]
    n = own.shape[0]
    least = jnp.array(-jnp.inf, own.dtype)
    spaced = [lax.pad(v, least, ((k * n, (3 - k) * n, 0), (0, 0, 0))) for k, v in enumerate(pieces)]
    return jnp.maximum(jnp.maximum(spaced[0], spaced[1]), jnp.maximum(spaced[2], spaced[3]))


def wide(value):
    return value.astype(jnp.float32)


def onward_kernel(spot, own_up, own_down, near_up, near_down, *rest):
    *turn, up, down = rest
    upward = wide(own_up[0]) + wide(near_up[0])
    downward = wide(own_down[0]) + wide(near_down[0])
    if turn:
        came = wide(turn[0][...])
        upward = upward + jnp.where(spot[2] == 1, came, 0.0)
        downward = downward + jnp.where(spot[2] == 1, 0.0, came)
    up[...] = upward.astype(up.dtype)
    down[...] = downward.astype(down.dtype)


def onward(blocks, near_up, near_down, *turn):
    here = lax.axis_index("depth")
    spot = jnp.stack([(here + 2) % 8, (here + 6) % 8, 1 - here % 2]).astype(jnp.int32)
    shape = blocks.shape[1:]
    block = lambda pick: pl.BlockSpec((1, *shape), pick)
    specs = [block(lambda i, s: (s[0], 0, 0)), block(lambda i, s: (s[1], 0, 0))]
    specs += [block(lambda i, s: (1, 0, 0))] * 2 + [pl.BlockSpec(shape, lambda i, s: (0, 0))] * len(turn)
    whole = pl.BlockSpec(memory_space=pltpu.VMEM)
    return pl.pallas_call(
        onward_kernel,
        out_shape=[pltpu.VMEM(shape, blocks.dtype)] * 2,
        grid_spec=pltpu.PrefetchScalarGridSpec(
            num_scalar_prefetch=1, grid=(1,), in_specs=specs, out_specs=[whole] * 2
        ),
        name="onward",
    )(spot, blocks, blocks, near_up, near_down, *turn)


def depth_parts(blocks, straight):
    here = lax.axis_index("depth")
    pick = lambda by: block_at(blocks, (here + by) % 8)
    near_up = shifted(jnp.stack([pick(1), pick(3)]), "depth", 1)
    near_down = shifted(jnp.stack([pick(7), pick(5)]), "depth", 7)
    if straight:
        far, turn = [shifted(pick(4), "depth", 4)], []
    else:
        turns = [(k, (k + 2) % 8 if k % 2 == 0 else (k - 2) % 8) for k in range(8)]
        far, turn = [], [lax.ppermute(pick(4), "depth", turns)]
    up, down = onward(blocks, near_up, near_down, *turn)
    last_up = shifted(up, "depth", 2)
    last_down = shifted(down, "depth", 6)
    near = wide(pick(0)) + wide(near_up[0]) + wide(near_down[0])
    return near, last_up, last_down, *far


def total(parts):
    return sum(wide(part) for part in parts)


def step(inputs, pre_act, grad_out, weight_up, weight_down):
    core = lax.axis_index("core")
    high = lax.axis_index("yhi")
    active, slope = gelu_parts(wide(pre_act[0]))
    active, slope = lax.optimization_barrier((active.astype(jnp.bfloat16), slope))
    active_mine = gathered(active)

    both = spread(jnp.concatenate([grad_out[0], inputs[0]], axis=1), COL)
    width = inputs.shape[2]
    both = both.reshape(4, 2, *both.shape[1:])
    of = lambda c: lax.dynamic_index_in_dim(both, c, 1, keepdims=False)
    mine, other = of(core), of(1 - core)
    flat = lambda blocks: blocks.reshape(-1, blocks.shape[-1])
    away = contract_last(flat(other[..., :width]), weight_down).astype(jnp.bfloat16)
    back = swapped(away)
    kept = lax.optimization_barrier(contract_last(flat(mine[..., :width]), weight_down))
    pair = (kept + wide(back)).astype(jnp.bfloat16).reshape(4, 64, -1)
    came = exchanged(pair, "yhi")

    active_other = swapped(active_mine)
    turned = lambda blocks: jnp.concatenate([block_at(blocks, (high + u) % 4) for u in range(4)], axis=0)
    lower_mine = lax.optimization_barrier(contract_first(active_mine, turned(mine[..., :width])))
    lower = contract_first(active_other, turned(other[..., :width])) + lower_mine
    lower = lower.astype(jnp.bfloat16)
    lower_parts = depth_parts(lower.reshape(8, -1, lower.shape[1]), True)

    delta_own = (sum(wide(came[k]) for k in range(4)) * slope).astype(jnp.bfloat16)
    delta_mine = flat(spread(delta_own, "yhi"))
    delta_other = swapped(delta_mine)

    late, _ = lax.optimization_barrier((other, pair))
    inputs_other = lax.optimization_barrier(late[..., width:])
    upper_mine = lax.optimization_barrier(contract_first(delta_mine, flat(mine[..., width:])))
    upper = contract_first(delta_other, flat(inputs_other)) + upper_mine
    upper = upper.astype(jnp.bfloat16)
    near, last_up, last_down = depth_parts(upper.reshape(8, -1, upper.shape[1]), False)

    parts_mine = contract_last(delta_mine, weight_up).astype(jnp.bfloat16)
    parts_other = contract_last(delta_other, weight_up).astype(jnp.bfloat16)
    first = jnp.where(core == 0, parts_mine, parts_other).reshape(4, 64, -1)
    second = jnp.where(core == 0, parts_other, parts_mine).reshape(4, 64, -1)
    parts = jnp.stack([first, second], axis=1).reshape(8, 64, -1)
    parts = exchanged(parts, COL)
    grad_inputs = summed(parts).astype(jnp.bfloat16)[None]
    grad_down = total(lower_parts)
    grad_inputs, grad_down, last_up = lax.optimization_barrier((grad_inputs, grad_down, last_up))
    grad_up = total((near, last_up, last_down))
    return (grad_inputs, grad_up.T, grad_down)


def solution(mesh):
    fine = Mesh(mesh.devices.reshape(4, 2, 2, 4, 8), ("yhi", "core", "ylo", "x", "depth"))
    placed = (
        P("depth", COL, ROW),
        P("depth", ROW, COL),
        P("depth", COL, ROW),
        P(ROW, COL),
        P(COL, ROW),
    )
    return jax.shard_map(
        step,
        mesh=fine,
        in_specs=placed,
        out_specs=(
            P("depth", COL, ROW),
            P(ROW, (*COL, "depth")),
            P((*COL, "depth"), ROW),
        ),
        check_vma=False,
    )
```
